32 devices in a mesh: rows: 8 (over y, x, core), rhs: 4 (over z).
Axes of the slice: x: 2, y: 2, z: 4, core: 2. Of those that a mesh axis runs over, the one named last changes fastest.
Arguments:
- sources: bfloat16 [32768, 2048], P('rows', 'rhs'), may hold values from -6 to 6
- near_blocks: bfloat16 [128, 3, 256, 256], P('rows'), may hold values from -0.21875 to 0.21875
- near_list: int32 [128, 3], P('rows'), may hold values from 0 to 127, as said below
- source_basis: bfloat16 [128, 256, 32], P('rows'), may hold values from -0.375 to 0.375
- target_basis: bfloat16 [128, 256, 32], P('rows'), may hold values from -0.375 to 0.375
- transfer_fine: bfloat16 [224, 32, 32], P('rows'), may hold values from -0.875 to 0.875
- transfer_coarse: bfloat16 [32, 32, 32], P('rhs'), may hold values from -0.875 to 0.875
- couple_fine: bfloat16 [224, 3, 32, 32], P('rows'), may hold values from -0.625 to 0.625
- couple_coarse: bfloat16 [32, 3, 32, 32], P('rhs'), may hold values from -0.625 to 0.625
- far_fine: int32 [224, 3], P('rows'), may hold values from 0 to 127, as said below
- far_coarse: int32 [32, 3], replicated, may hold values from -1 to 15, as said below
Outputs:
- potentials: bfloat16 [32768, 2048], P('rows', 'rhs')
The draws below stay inside these ranges and needn't reach their ends.
Inputs may be any that keep to these rules, and one draw needn't show every extreme that they name: `near_list`: row t lists the leaf clusters t - 1, t and t + 1 modulo 128 in some order. `far_fine`: row d * 28 + o + i belongs to cluster d * m + i of the level with n = m * 8 clusters, where (o, m) is (0, 16), (16, 8) or (24, 4). It lists, in some order, the three clusters of that level that are children of the cyclic neighbours of the cluster's parent and not cyclic neighbours of the cluster: for cluster j with parent p = j // 2, the clusters 2p - 2, 2p + 2, 2p + 3 if j is even and 2p - 2, 2p - 1, 2p + 3 if j is odd, modulo n. `far_coarse`: row n + j for n = 8, 16, ..., 16 lists, in some order, the three far clusters of cluster j of the level with n clusters by the rule of far_fine. Row 4 + j holds (j + 2) modulo 4 in slot 0 and -1 in slots 1 and 2. Rows 0 to 3 hold -1.
All inputs are finite; a program needn't handle non-finite values.
Results may differ from the reference program's by a relative error of at most 0.012.
Values may be sent and summed in bfloat16 or wider, within the bound.
A program may use at most 128 MiB of HBM per device.

```python
import jax
import jax.numpy as jnp
from jax import lax

LEAF = 256
RANK = 32
LPD = 16
LEAVES = 128
POINTS = 32768
RHS = 2048
FINE = 224
COARSE = 32


def shuffle_rows(key, table):
    keys = jax.random.split(key, table.shape[0])

    def one_order(single):
        return jax.random.permutation(single, 3)
    orders = jax.vmap(one_order)(keys)
    return jnp.take_along_axis(table, orders, axis=1)


def far_rule(index, clusters):
    parent = index // 2
    second = jnp.where(index % 2 == 1, 2 * parent - 1, 2 * parent + 2)
    first = (2 * parent - 2 + 4 * clusters) % clusters
    second = (second + 4 * clusters) % clusters
    third = (2 * parent + 3) % clusters
    return jnp.stack([first, second, third], axis=1).astype(jnp.int32)


def draw_near_list(key, part):
    leaves = jnp.arange(LEAVES, dtype=jnp.int32)
    table = jnp.stack([(leaves + LEAVES - 1) % LEAVES, leaves, (leaves + 1) % LEAVES], axis=1)
    return shuffle_rows(jax.random.fold_in(key, 11), table)


def draw_far_fine(key, part):
    row_count = LEAVES // LPD
    block = LPD + LPD // 2 + LPD // 4
    rows_all = jnp.arange(row_count * block, dtype=jnp.int32)
    device = rows_all // block
    within = rows_all % block
    local_count = jnp.where(within < LPD, LPD, jnp.where(within < LPD + LPD // 2, LPD // 2, LPD // 4))
    offset = jnp.where(within < LPD, 0, jnp.where(within < LPD + LPD // 2, LPD, LPD + LPD // 2))
    index = device * local_count + within - offset
    table = far_rule(index, local_count * row_count)
    return shuffle_rows(jax.random.fold_in(key, 23), table)


def draw_far_coarse(key, part):
    row_count = LEAVES // LPD
    empty = jnp.full((4,), -1, jnp.int32)
    top = jnp.arange(4, dtype=jnp.int32)
    pieces = [jnp.full((4, 3), -1, jnp.int32), jnp.stack([(top + 2) % 4, empty, empty], axis=1)]
    clusters = 8
    for level in range((2 * row_count).bit_length() - 3):
        index = jnp.arange(clusters, dtype=jnp.int32)
        pieces.append(shuffle_rows(jax.random.fold_in(key, 100 + clusters), far_rule(index, clusters)))
        clusters = clusters * 2
    return jnp.concatenate(pieces, axis=0)


def block_scale(own_key, dims, cuts, low, largest):
    def one(position, parts):
        heights = jax.random.uniform(jax.random.fold_in(jax.random.fold_in(own_key, 6), position), (parts,), jnp.float32, low / len(cuts), largest / len(cuts))
        return jnp.repeat(jnp.exp(heights), dims[position] // parts).reshape((-1,) + (1,) * (len(dims) - position - 1))

    gain = one(*cuts[0])
    for cut in cuts[1:]:
        gain = gain * one(*cut)
    return gain


def centred(stream_key, extent, deviation, most, shards=(), held_as=jnp.bfloat16):
    gain = block_scale(stream_key, extent, shards, -0.22, 0.18) if shards else 1.0
    values = jax.random.normal(stream_key, extent, jnp.float32) * deviation * gain
    return jnp.minimum(jnp.maximum(values, -most), most).astype(held_as)


def setup_inputs(seed: int = 0) -> dict:
    splits = jax.random.split(jax.random.key(seed), 12)
    sources = centred(splits[0], (POINTS, RHS), 1.0, 6.0, ((0, 8), (1, 4)))
    near_blocks = centred(splits[1], (LEAVES, 3, LEAF, LEAF), (3 * LEAF) ** -0.5, 0.21875, ((0, 8),))
    near_list = draw_near_list(jax.random.fold_in(splits[11], 71), 0)
    source_basis = centred(splits[3], (LEAVES, LEAF, RANK), LEAF ** -0.5, 0.375, ((0, 8),))
    target_basis = centred(splits[4], (LEAVES, LEAF, RANK), (8 * RANK) ** -0.5, 0.375, ((0, 8),))
    transfer_fine = centred(splits[5], (FINE, RANK, RANK), (3 * RANK // 2) ** -0.5, 0.875, ((0, 8),))
    transfer_coarse = centred(splits[6], (COARSE, RANK, RANK), (3 * RANK // 2) ** -0.5, 0.875, ((0, 4),))
    couple_fine = centred(splits[7], (FINE, 3, RANK, RANK), (3 * RANK) ** -0.5, 0.625, ((0, 8),))
    couple_coarse = centred(splits[8], (COARSE, 3, RANK, RANK), (3 * RANK) ** -0.5, 0.625, ((0, 4),))
    far_fine = draw_far_fine(jax.random.fold_in(splits[11], 71), 0)
    far_coarse = draw_far_coarse(jax.random.fold_in(splits[11], 71), 0)
    return dict(sources=sources, near_blocks=near_blocks, near_list=near_list, source_basis=source_basis, target_basis=target_basis, transfer_fine=transfer_fine, transfer_coarse=transfer_coarse, couple_fine=couple_fine, couple_coarse=couple_coarse, far_fine=far_fine, far_coarse=far_coarse)


def fine_level(table, row_count, first, count):
    block = table.shape[0] // row_count
    shaped = table.reshape((row_count, block) + table.shape[1:])
    return shaped[:, first:first + count].reshape((row_count * count,) + table.shape[1:])


def couple(moments, blocks, partners):
    valid = partners >= 0
    picked = moments[jnp.maximum(partners, 0)]
    picked = jnp.where(valid[:, :, None, None], picked, jnp.zeros_like(picked))
    return jnp.einsum('nsab,nsbr->nar', blocks.astype(jnp.float32), picked.astype(jnp.float32))


def lift(moments, transfer):
    clusters, rank, width = moments.shape
    product = jnp.einsum('nab,nar->nbr', transfer.astype(jnp.float32), moments.astype(jnp.float32))
    return product.reshape(clusters // 2, 2, rank, width).sum(axis=1).astype(jnp.bfloat16)


def lower(parent, transfer, coupled):
    spread = jnp.repeat(parent, 2, axis=0)
    carried = jnp.einsum('nab,nbr->nar', transfer.astype(jnp.float32), spread.astype(jnp.float32))
    return (coupled + carried).astype(jnp.bfloat16)


def reference(sources, near_blocks, near_list, source_basis, target_basis, transfer_fine, transfer_coarse, couple_fine, couple_coarse, far_fine, far_coarse):
    row_count = LEAVES // LPD
    width = sources.shape[1]
    counts = [LPD, LPD // 2, LPD // 4]
    firsts = [0, LPD, LPD + LPD // 2]
    shaped = sources.reshape(LEAVES, LEAF, width)

    def leaf_moments(index):
        return jnp.dot(source_basis[index].T, shaped[index], preferred_element_type=jnp.float32).astype(jnp.bfloat16)

    moments = lax.map(leaf_moments, jnp.arange(LEAVES, dtype=jnp.int32))
    upward = [moments]
    fine_tables = []
    for level in range(3):
        transfer = fine_level(transfer_fine, row_count, firsts[level], counts[level])
        blocks = fine_level(couple_fine, row_count, firsts[level], counts[level])
        partners = fine_level(far_fine, row_count, firsts[level], counts[level])
        fine_tables.append((transfer, blocks, partners))
        moments = lift(moments, transfer)
        upward.append(moments)
    clusters = 2 * row_count
    depth = clusters.bit_length() - 3
    coarse_up = [moments]
    for step in range(depth):
        moments = lift(moments, transfer_coarse[clusters:2 * clusters])
        clusters = clusters // 2
        coarse_up.append(moments)
    downward = moments
    for step in range(depth + 1):
        coupled = couple(coarse_up[depth - step], couple_coarse[clusters:2 * clusters], far_coarse[clusters:2 * clusters])
        if step == 0:
            downward = coupled.astype(jnp.bfloat16)
        else:
            downward = lower(downward, transfer_coarse[clusters:2 * clusters], coupled)
        clusters = clusters * 2
    for level in (2, 1, 0):
        transfer, blocks, partners = fine_tables[level]
        coupled = couple(upward[level], blocks, partners)
        downward = lower(downward, transfer, coupled)

    def leaf_output(index):
        summed = jnp.dot(target_basis[index], downward[index], preferred_element_type=jnp.float32)
        for slot in range(3):
            summed = summed + jnp.dot(near_blocks[index, slot], shaped[near_list[index, slot]], preferred_element_type=jnp.float32)
        return summed.astype(jnp.bfloat16)

    result = lax.map(leaf_output, jnp.arange(LEAVES, dtype=jnp.int32))
    return result.reshape(LEAVES * LEAF, width)
```

```python
import jax
import jax.numpy as jnp
from jax import lax
from jax.experimental import pallas as pl
from jax.experimental.pallas import tpu as pltpu
from jax.sharding import PartitionSpec as P

MESH = pl.DeviceIdType.MESH
F32 = jnp.float32
BF16 = jnp.bfloat16


def dot(a, b):
    return lax.dot_general(a, b, (((1,), (0,)), ((), ())), preferred_element_type=F32)


def dot_t(a, b):
    return lax.dot_general(a, b, (((0,), (0,)), ((), ())), preferred_element_type=F32)


def kernel(
    dims,
    x_hbm,
    near_hbm,
    near_list,
    sb_hbm,
    tb_hbm,
    ef_hbm,
    ec_hbm,
    sf_hbm,
    sc_hbm,
    far_fine,
    far_coarse,
    out_hbm,
    xw,
    near,
    sb,
    tb,
    ef,
    ec,
    sf,
    sc,
    wf,
    wc,
    cw0,
    cw1,
    cw2,
    cw3,
    cr,
    cu,
    fr,
    f3,
    f2,
    f1,
    f0,
    part,
    obuf,
    load_sem,
    out_sem,
    halo_send,
    halo_recv,
    table_send,
    table_recv,
    gather_send,
    gather_recv,
):
    count, leaf, rank, R, T, chunks = dims
    me = lax.axis_index("rows")
    z = lax.axis_index("rhs")
    right, left = lax.rem(me + 1, R), lax.rem(me + R - 1, R)
    per = count // chunks
    block = ec.shape[0]

    loads = [
        pltpu.make_async_copy(ec_hbm, ec, load_sem.at[0]),
        pltpu.make_async_copy(sc_hbm, sc, load_sem.at[1]),
        pltpu.make_async_copy(sb_hbm, sb, load_sem.at[2]),
    ]
    x_loads = [
        pltpu.make_async_copy(
            x_hbm.at[pl.ds(c * per, per)], xw.at[pl.ds(1 + c * per, per)], load_sem.at[7 + c]
        )
        for c in range(chunks)
    ]
    late = [
        pltpu.make_async_copy(ef_hbm, ef, load_sem.at[3]),
        pltpu.make_async_copy(sf_hbm, sf, load_sem.at[4]),
        pltpu.make_async_copy(near_hbm, near, load_sem.at[5]),
        pltpu.make_async_copy(tb_hbm, tb, load_sem.at[6]),
    ]
    for copy in loads + x_loads + late:
        copy.start()

    barrier = pltpu.get_barrier_semaphore()
    for k in range(1, R):
        pl.semaphore_signal(
            barrier, inc=1, device_id=(lax.rem(me + k, R), z), device_id_type=MESH
        )
    for k in range(1, T):
        pl.semaphore_signal(
            barrier, inc=1, device_id=(me, lax.rem(z + k, T)), device_id_type=MESH
        )

    loads[0].wait()
    loads[1].wait()
    for r in range(block):
        wc[z * block + r] = jnp.concatenate([sc[r, 0], sc[r, 1], sc[r, 2], ec[r]], axis=1)
    pl.semaphore_wait(barrier, R + T - 2)

    def send(src, dst, send_sem, recv_sem, row, col):
        return pltpu.make_async_remote_copy(
            src_ref=src,
            dst_ref=dst,
            send_sem=send_sem,
            recv_sem=recv_sem,
            device_id=(row, col),
            device_id_type=MESH,
        )

    mine = wc.at[pl.ds(z * block, block)]
    tables = []
    for k in range(1, T):
        copy = send(
            mine, mine, table_send.at[k], table_recv.at[z], me, lax.rem(z + k, T)
        )
        copy.start()
        tables.append(copy)

    def halo(ref, width, size, level):
        low = send(
            ref.at[pl.ds(width, width)],
            ref.at[pl.ds(width + size, width)],
            halo_send.at[2 * level],
            halo_recv.at[2 * level],
            left,
            z,
        )
        high = send(
            ref.at[pl.ds(size, width)],
            ref.at[pl.ds(0, width)],
            halo_send.at[2 * level + 1],
            halo_recv.at[2 * level + 1],
            right,
            z,
        )
        low.start()
        high.start()
        return [low, high]

    loads[2].wait()
    for c in range(chunks):
        x_loads[c].wait()
        for t in range(c * per, (c + 1) * per):
            cw0[2 + t] = dot(sb[t], xw[1 + t]).astype(BF16)
    windows = [cw0, cw1, cw2, cw3]
    sizes = [count, count // 2, count // 4, count // 8]
    firsts = [0, count, count + count // 2]
    halos = [halo(cw0, 2, count, 0)]
    late[0].wait()
    for level in range(3):
        below, above = windows[level], windows[level + 1]
        for j in range(sizes[level + 1]):
            pair = below[2 + 2 * j : 4 + 2 * j].reshape(2 * rank, -1)
            first = firsts[level] + 2 * j
            matrix = ef[first : first + 2].reshape(2 * rank, rank)
            above[2 + j] = dot_t(matrix, pair).astype(BF16)
        halos.append(halo(above, 2, sizes[level + 1], level + 1))

    for k in range(1, T):
        other = lax.rem(z + k, T)
        theirs = wc.at[pl.ds(other * block, block)]
        send(theirs, theirs, table_send.at[k], table_recv.at[other], me, other).wait_recv()

    def transfer(row):
        return wc[row][:, 3 * rank :]

    own = dot_t(transfer(2 * R + 2 * me), cw3[2]) + dot_t(transfer(2 * R + 2 * me + 1), cw3[3])
    cr[me] = own.astype(BF16)
    gathers = []
    for k in range(1, R):
        spot = cr.at[pl.ds(me, 1)]
        copy = send(
            spot, spot, gather_send.at[k], gather_recv.at[me], lax.rem(me + k, R), z
        )
        copy.start()
        gathers.append(copy)
    halos.append(halo(xw, 1, count, 4))

    late[1].wait()
    for j in range(wf.shape[0]):
        wf[j] = jnp.concatenate([sf[j, 0], sf[j, 1], sf[j, 2], ef[j]], axis=1)

    total = count * R
    late[2].wait()

    def near_leaf(t):
        total_sum = None
        for wanted in (-1, 0, 1):
            target = lax.rem(me * count + t + wanted + total, total)
            slot = jnp.where(
                near_list[0, t] == target, 0, jnp.where(near_list[1, t] == target, 1, 2)
            )
            term = dot(near[t, slot], xw[1 + t + wanted])
            total_sum = term if total_sum is None else total_sum + term
        return total_sum

    def near_step(i, carry):
        for u in range(2):
            t = 1 + 2 * i + u
            part[t] = near_leaf(t)
        return carry

    lax.fori_loop(0, (count - 2) // 2, near_step, 0)

    for k in range(1, R):
        other = lax.rem(me + k, R)
        spot = cr.at[pl.ds(other, 1)]
        send(spot, spot, gather_send.at[k], gather_recv.at[other], other, z).wait_recv()

    def coarse(n, index):
        return cr[index] if n == R else cu[n - 4 + index]

    n = R // 2
    while n >= 4:
        for j in range(n):
            lifted = dot_t(transfer(2 * n + 2 * j), coarse(2 * n, 2 * j)) + dot_t(
                transfer(2 * n + 2 * j + 1), coarse(2 * n, 2 * j + 1)
            )
            cu[n - 4 + j] = lifted.astype(BF16)
        n //= 2
    n = 4
    value = None
    while n <= R:
        row = n + me // (R // n)
        if n == 4:
            value = dot(wc[row][:, :rank], coarse(n, far_coarse[0, row]))
        else:
            parts = [coarse(n, far_coarse[s, row]) for s in range(3)] + [value]
            value = dot(wc[row], jnp.concatenate(parts, axis=0))
        value = value.astype(BF16)
        n *= 2
    fr[0] = value

    def wait_halo(level):
        for copy in halos[level]:
            copy.wait_recv()

    wait_halo(3)
    for i in range(2):
        row = 2 * R + 2 * me + i
        parts = [
            cw3[jnp.minimum(lax.rem(far_coarse[s, row] - 2 * me + 2 + 2 * R, 2 * R), 5)]
            for s in range(3)
        ] + [fr[0]]
        f3[i] = dot(wc[row], jnp.concatenate(parts, axis=0)).astype(BF16)
    above = f3
    for level, below in ((2, f2), (1, f1), (0, f0)):
        wait_halo(level)
        m = sizes[level]
        n = m * R
        for i in range(m):
            row = firsts[level] + i
            parts = [
                windows[level][jnp.minimum(lax.rem(far_fine[s, row] - m * me + 2 + n, n), m + 3)]
                for s in range(3)
            ] + [above[i // 2]]
            below[i] = dot(wf[row], jnp.concatenate(parts, axis=0)).astype(BF16)
        above = below

    late[3].wait()
    wait_halo(4)
    part[0] = near_leaf(0)
    part[count - 1] = near_leaf(count - 1)
    stores = []
    for c in range(chunks):
        for t in range(c * per, (c + 1) * per):
            obuf[t] = (part[t] + dot_t(tb[t], f0[t])).astype(BF16)
        copy = pltpu.make_async_copy(
            obuf.at[pl.ds(c * per, per)], out_hbm.at[pl.ds(c * per, per)], out_sem.at[c]
        )
        copy.start()
        stores.append(copy)
    for copy in tables + gathers:
        copy.wait_send()
    for pair in halos:
        for copy in pair:
            copy.wait_send()
    for copy in stores:
        copy.wait()


def body(
    sources,
    near_blocks,
    near_list,
    source_basis,
    target_basis,
    transfer_fine,
    transfer_coarse,
    couple_fine,
    couple_coarse,
    far_fine,
    far_coarse,
):
    count, _, leaf, _ = near_blocks.shape
    rank = source_basis.shape[2]
    width = sources.shape[1]
    R, T = lax.axis_size("rows"), lax.axis_size("rhs")
    fine = transfer_fine.shape[0]
    block = transfer_coarse.shape[0]
    chunks = 4
    dims = (count, leaf, rank, R, T, chunks)
    anyspace = pl.BlockSpec(memory_space=pl.ANY)
    smem = pl.BlockSpec(memory_space=pltpu.SMEM)

    def moments(clusters):
        return pltpu.VMEM((clusters, rank, width), BF16)

    out = pl.pallas_call(
        lambda *refs: kernel(dims, *refs),
        name="tree_apply",
        out_shape=jax.ShapeDtypeStruct((count, leaf, width), BF16),
        in_specs=[
            anyspace,
            anyspace,
            smem,
            anyspace,
            anyspace,
            anyspace,
            anyspace,
            anyspace,
            anyspace,
            smem,
            smem,
        ],
        out_specs=anyspace,
        scratch_shapes=[
            pltpu.VMEM((count + 2, leaf, width), BF16),
            pltpu.VMEM(near_blocks.shape, BF16),
            pltpu.VMEM((count, rank, leaf), BF16),
            pltpu.VMEM((count, rank, leaf), BF16),
            pltpu.VMEM(transfer_fine.shape, BF16),
            pltpu.VMEM(transfer_coarse.shape, BF16),
            pltpu.VMEM(couple_fine.shape, BF16),
            pltpu.VMEM(couple_coarse.shape, BF16),
            pltpu.VMEM((fine, rank, 4 * rank), BF16),
            pltpu.VMEM((block * T, rank, 4 * rank), BF16),
            moments(count + 4),
            moments(count // 2 + 4),
            moments(count // 4 + 4),
            moments(count // 8 + 4),
            moments(R),
            moments(R),
            moments(1),
            moments(count // 8),
            moments(count // 4),
            moments(count // 2),
            moments(count),
            pltpu.VMEM((count, leaf, width), F32),
            pltpu.VMEM((count, leaf, width), BF16),
            pltpu.SemaphoreType.DMA((7 + chunks,)),
            pltpu.SemaphoreType.DMA((chunks,)),
            pltpu.SemaphoreType.DMA((10,)),
            pltpu.SemaphoreType.DMA((10,)),
            pltpu.SemaphoreType.DMA((T,)),
            pltpu.SemaphoreType.DMA((T,)),
            pltpu.SemaphoreType.DMA((R,)),
            pltpu.SemaphoreType.DMA((R,)),
        ],
        compiler_params=pltpu.CompilerParams(
            collective_id=0, has_side_effects=True, vmem_limit_bytes=56 * 1024 * 1024
        ),
    )(
        sources.reshape(count, leaf, width),
        near_blocks,
        near_list.T,
        jnp.swapaxes(source_basis, 1, 2),
        jnp.swapaxes(target_basis, 1, 2),
        transfer_fine,
        transfer_coarse,
        couple_fine,
        couple_coarse,
        far_fine.T,
        far_coarse.T,
    )
    return out.reshape(count * leaf, width)


def solution(mesh):
    in_specs = (
        P("rows", "rhs"),
        P("rows", None, None, None),
        P("rows", None),
        P("rows", None, None),
        P("rows", None, None),
        P("rows", None, None),
        P("rhs", None, None),
        P("rows", None, None, None),
        P("rhs", None, None, None),
        P("rows", None),
        P(),
    )
    out_specs = P("rows", "rhs")
    return jax.shard_map(body, mesh=mesh, in_specs=in_specs, out_specs=out_specs, check_vma=False)
```

```python
import jax
import jax.numpy as jnp
from jax import lax
from jax.experimental import pallas as pl
from jax.experimental.pallas import tpu as pltpu
from jax.sharding import PartitionSpec as P

MESH = pl.DeviceIdType.MESH
F32 = jnp.float32
BF16 = jnp.bfloat16


def dot(a, b):
    return lax.dot_general(a, b, (((1,), (0,)), ((), ())), preferred_element_type=F32)


def dot_t(a, b):
    return lax.dot_general(a, b, (((0,), (0,)), ((), ())), preferred_element_type=F32)


def kernel(
    dims,
    x_hbm,
    near_hbm,
    near_list,
    sb_hbm,
    ef_hbm,
    ec_hbm,
    sf_hbm,
    sc_hbm,
    far_fine,
    far_coarse,
    part_hbm,
    f_hbm,
    xw,
    near,
    sb,
    ef,
    ec,
    sf,
    sc,
    wf,
    wc,
    cw0,
    cw1,
    cw2,
    cw3,
    cr,
    cu,
    fr,
    f3,
    f2,
    f1,
    f0,
    part,
    load_sem,
    out_sem,
    halo_send,
    halo_recv,
    table_send,
    table_recv,
    gather_send,
    gather_recv,
    pair_send,
    pair_recv,
):
    count, leaf, rank, R, T, chunks = dims
    me = lax.axis_index("rows")
    z = lax.axis_index("rhs")
    right, left = lax.rem(me + 1, R), lax.rem(me + R - 1, R)
    per = count // chunks
    block = ec.shape[0]

    loads = [
        pltpu.make_async_copy(ec_hbm, ec, load_sem.at[0]),
        pltpu.make_async_copy(sc_hbm, sc, load_sem.at[1]),
        pltpu.make_async_copy(sb_hbm, sb, load_sem.at[2]),
    ]
    x_loads = [
        pltpu.make_async_copy(
            x_hbm.at[pl.ds(c * per, per)], xw.at[pl.ds(1 + c * per, per)], load_sem.at[7 + c]
        )
        for c in range(chunks)
    ]
    late = [
        pltpu.make_async_copy(ef_hbm, ef, load_sem.at[3]),
        pltpu.make_async_copy(sf_hbm, sf, load_sem.at[4]),
        pltpu.make_async_copy(near_hbm, near, load_sem.at[5]),
    ]
    for copy in loads + x_loads + late[:2]:
        copy.start()

    barrier = pltpu.get_barrier_semaphore()
    for k in range(1, R):
        pl.semaphore_signal(
            barrier, inc=1, device_id=(lax.rem(me + k, R), z), device_id_type=MESH
        )
    for k in range(1, T):
        pl.semaphore_signal(
            barrier, inc=1, device_id=(me, lax.rem(z + k, T)), device_id_type=MESH
        )

    loads[0].wait()
    loads[1].wait()
    for r in range(block):
        wc[z * block + r] = jnp.concatenate([sc[r, 0], sc[r, 1], sc[r, 2], ec[r]], axis=1)
    pl.semaphore_wait(barrier, R + T - 2)

    def send(src, dst, send_sem, recv_sem, row, col):
        return pltpu.make_async_remote_copy(
            src_ref=src,
            dst_ref=dst,
            send_sem=send_sem,
            recv_sem=recv_sem,
            device_id=(row, col),
            device_id_type=MESH,
        )

    low = send(
        x_hbm.at[pl.ds(0, 1)],
        xw.at[pl.ds(count + 1, 1)],
        halo_send.at[8],
        halo_recv.at[8],
        left,
        z,
    )
    high = send(
        x_hbm.at[pl.ds(count - 1, 1)],
        xw.at[pl.ds(0, 1)],
        halo_send.at[9],
        halo_recv.at[9],
        right,
        z,
    )
    low.start()
    high.start()
    edges = [low, high]

    pair_rows = wc.at[pl.ds(2 * R + 2 * me, 2)]
    pair_owner = (2 * R + 2 * me) // block
    coarse_blocks = (2 * R + block - 1) // block
    mine = wc.at[pl.ds(z * block, block)]

    def pair_copy(k, source, target):
        return send(pair_rows, pair_rows, pair_send.at[k], pair_recv.at[source], me, target)

    def table_copy(k, source, target):
        return send(mine, mine, table_send.at[k], table_recv.at[source], me, target)

    @pl.when(z == pair_owner)
    def _():
        for k in range(1, T):
            pair_copy(k, z, lax.rem(z + k, T)).start()

    @pl.when(z < coarse_blocks)
    def _():
        for k in range(1, T):
            table_copy(k, z, lax.rem(z + k, T)).start()

    def halo(ref, width, size, level):
        low = send(
            ref.at[pl.ds(width, width)],
            ref.at[pl.ds(width + size, width)],
            halo_send.at[2 * level],
            halo_recv.at[2 * level],
            left,
            z,
        )
        high = send(
            ref.at[pl.ds(size, width)],
            ref.at[pl.ds(0, width)],
            halo_send.at[2 * level + 1],
            halo_recv.at[2 * level + 1],
            right,
            z,
        )
        low.start()
        high.start()
        return [low, high]

    loads[2].wait()
    for c in range(chunks):
        x_loads[c].wait()
    late[2].start()
    for c in range(chunks):
        for t in range(c * per, (c + 1) * per):
            cw0[2 + t] = dot(sb[t], xw[1 + t]).astype(BF16)
    windows = [cw0, cw1, cw2, cw3]
    sizes = [count, count // 2, count // 4, count // 8]
    firsts = [0, count, count + count // 2]
    late[0].wait()
    for level in range(3):
        below, above = windows[level], windows[level + 1]
        for j in range(sizes[level + 1]):
            pair = below[2 + 2 * j : 4 + 2 * j].reshape(2 * rank, -1)
            first = firsts[level] + 2 * j
            matrix = ef[first : first + 2].reshape(2 * rank, rank)
            above[2 + j] = dot_t(matrix, pair).astype(BF16)

    @pl.when(z != pair_owner)
    def _():
        pair_copy(0, pair_owner, lax.rem(z + 1, T)).wait_recv()

    def transfer(row):
        return wc[row][:, 3 * rank :]

    own = dot_t(transfer(2 * R + 2 * me), cw3[2]) + dot_t(transfer(2 * R + 2 * me + 1), cw3[3])
    cr[me] = own.astype(BF16)
    gathers = []
    for k in range(1, R):
        spot = cr.at[pl.ds(me, 1)]
        copy = send(
            spot, spot, gather_send.at[k], gather_recv.at[me], lax.rem(me + k, R), z
        )
        copy.start()
        gathers.append(copy)
    halos = [None] * 4
    for level in (3, 2, 1, 0):
        halos[level] = halo(windows[level], 2, sizes[level], level)

    late[1].wait()
    for j in range(wf.shape[0]):
        wf[j] = jnp.concatenate([sf[j, 0], sf[j, 1], sf[j, 2], ef[j]], axis=1)

    total = count * R
    late[2].wait()

    def near_leaf(t):
        total_sum = None
        for wanted in (-1, 0, 1):
            target = lax.rem(me * count + t + wanted + total, total)
            slot = jnp.where(
                near_list[0, t] == target, 0, jnp.where(near_list[1, t] == target, 1, 2)
            )
            term = dot(near[t, slot], xw[1 + t + wanted])
            total_sum = term if total_sum is None else total_sum + term
        return total_sum

    def near_step(i, carry):
        for u in range(2):
            t = 1 + 2 * i + u
            part[t] = near_leaf(t).astype(BF16)
        return carry

    lax.fori_loop(0, (count - 2) // 2, near_step, 0)
    stores = [
        pltpu.make_async_copy(
            part.at[pl.ds(1, count - 2)], part_hbm.at[pl.ds(1, count - 2)], out_sem.at[0]
        ),
        pltpu.make_async_copy(part.at[pl.ds(0, 1)], part_hbm.at[pl.ds(0, 1)], out_sem.at[1]),
        pltpu.make_async_copy(
            part.at[pl.ds(count - 1, 1)], part_hbm.at[pl.ds(count - 1, 1)], out_sem.at[2]
        ),
    ]
    stores[0].start()
    edges[0].wait_recv()
    part[count - 1] = near_leaf(count - 1).astype(BF16)
    edges[1].wait_recv()
    part[0] = near_leaf(0).astype(BF16)
    stores[1].start()
    stores[2].start()

    for k in range(1, R):
        other = lax.rem(me + k, R)
        spot = cr.at[pl.ds(other, 1)]
        send(spot, spot, gather_send.at[k], gather_recv.at[other], other, z).wait_recv()

    for k in range(1, T):
        other = lax.rem(z + k, T)
        theirs = wc.at[pl.ds(other * block, block)]

        @pl.when(other < coarse_blocks)
        def _():
            send(theirs, theirs, table_send.at[0], table_recv.at[other], me, other).wait_recv()

    def coarse(n, index):
        return cr[index] if n == R else cu[n - 4 + index]

    n = R // 2
    while n >= 4:
        for j in range(n):
            lifted = dot_t(transfer(2 * n + 2 * j), coarse(2 * n, 2 * j)) + dot_t(
                transfer(2 * n + 2 * j + 1), coarse(2 * n, 2 * j + 1)
            )
            cu[n - 4 + j] = lifted.astype(BF16)
        n //= 2
    n = 4
    value = None
    while n <= R:
        row = n + me // (R // n)
        if n == 4:
            value = dot(wc[row][:, :rank], coarse(n, far_coarse[0, row]))
        else:
            parts = [coarse(n, far_coarse[s, row]) for s in range(3)] + [value]
            value = dot(wc[row], jnp.concatenate(parts, axis=0))
        value = value.astype(BF16)
        n *= 2
    fr[0] = value

    def wait_halo(level):
        for copy in halos[level]:
            copy.wait_recv()

    wait_halo(3)
    for i in range(2):
        row = 2 * R + 2 * me + i
        parts = [
            cw3[jnp.minimum(lax.rem(far_coarse[s, row] - 2 * me + 2 + 2 * R, 2 * R), 5)]
            for s in range(3)
        ] + [fr[0]]
        f3[i] = dot(wc[row], jnp.concatenate(parts, axis=0)).astype(BF16)
    above = f3
    for level, below in ((2, f2), (1, f1), (0, f0)):
        wait_halo(level)
        m = sizes[level]
        n = m * R
        for i in range(m):
            row = firsts[level] + i
            parts = [
                windows[level][jnp.minimum(lax.rem(far_fine[s, row] - m * me + 2 + n, n), m + 3)]
                for s in range(3)
            ] + [above[i // 2]]
            below[i] = dot(wf[row], jnp.concatenate(parts, axis=0)).astype(BF16)
        above = below

    last = pltpu.make_async_copy(f0, f_hbm, out_sem.at[3])
    last.start()

    @pl.when(z == pair_owner)
    def _():
        for k in range(1, T):
            pair_copy(k, z, lax.rem(z + k, T)).wait_send()

    @pl.when(z < coarse_blocks)
    def _():
        for k in range(1, T):
            table_copy(k, z, lax.rem(z + k, T)).wait_send()

    for copy in gathers + edges:
        copy.wait_send()
    for pair in halos:
        for copy in pair:
            copy.wait_send()
    for copy in stores:
        copy.wait()
    last.wait()


def finish(part, tb, f, out):
    for t in range(part.shape[0]):
        out[t] = (part[t].astype(F32) + dot_t(tb[t], f[t])).astype(BF16)


def body(
    sources,
    near_blocks,
    near_list,
    source_basis,
    target_basis,
    transfer_fine,
    transfer_coarse,
    couple_fine,
    couple_coarse,
    far_fine,
    far_coarse,
):
    count, _, leaf, _ = near_blocks.shape
    rank = source_basis.shape[2]
    width = sources.shape[1]
    R, T = lax.axis_size("rows"), lax.axis_size("rhs")
    fine = transfer_fine.shape[0]
    block = transfer_coarse.shape[0]
    chunks = 4
    dims = (count, leaf, rank, R, T, chunks)
    anyspace = pl.BlockSpec(memory_space=pl.ANY)
    smem = pl.BlockSpec(memory_space=pltpu.SMEM)

    def moments(clusters):
        return pltpu.VMEM((clusters, rank, width), BF16)

    part, far = pl.pallas_call(
        lambda *refs: kernel(dims, *refs),
        name="tree_apply",
        out_shape=[
            jax.ShapeDtypeStruct((count, leaf, width), BF16),
            jax.ShapeDtypeStruct((count, rank, width), BF16),
        ],
        in_specs=[anyspace] * 2 + [smem] + [anyspace] * 5 + [smem] * 2,
        out_specs=[anyspace, anyspace],
        scratch_shapes=[
            pltpu.VMEM((count + 2, leaf, width), BF16),
            pltpu.VMEM(near_blocks.shape, BF16),
            pltpu.VMEM((count, rank, leaf), BF16),
            pltpu.VMEM(transfer_fine.shape, BF16),
            pltpu.VMEM(transfer_coarse.shape, BF16),
            pltpu.VMEM(couple_fine.shape, BF16),
            pltpu.VMEM(couple_coarse.shape, BF16),
            pltpu.VMEM((fine, rank, 4 * rank), BF16),
            pltpu.VMEM((block * T, rank, 4 * rank), BF16),
            moments(count + 4),
            moments(count // 2 + 4),
            moments(count // 4 + 4),
            moments(count // 8 + 4),
            moments(R),
            moments(R),
            moments(1),
            moments(count // 8),
            moments(count // 4),
            moments(count // 2),
            moments(count),
            pltpu.VMEM((count, leaf, width), BF16),
            pltpu.SemaphoreType.DMA((7 + chunks,)),
            pltpu.SemaphoreType.DMA((4,)),
            pltpu.SemaphoreType.DMA((10,)),
            pltpu.SemaphoreType.DMA((10,)),
            pltpu.SemaphoreType.DMA((T,)),
            pltpu.SemaphoreType.DMA((T,)),
            pltpu.SemaphoreType.DMA((R,)),
            pltpu.SemaphoreType.DMA((R,)),
            pltpu.SemaphoreType.DMA((T,)),
            pltpu.SemaphoreType.DMA((T,)),
        ],
        compiler_params=pltpu.CompilerParams(
            collective_id=0, has_side_effects=True, vmem_limit_bytes=63 * 1024 * 1024
        ),
    )(
        sources.reshape(count, leaf, width),
        near_blocks,
        near_list.T,
        jnp.swapaxes(source_basis, 1, 2),
        transfer_fine,
        transfer_coarse,
        couple_fine,
        couple_coarse,
        far_fine.T,
        far_coarse.T,
    )
    step = 4
    block_of = lambda *tail: pl.BlockSpec((step,) + tail, lambda i: (i, 0, 0))
    out = pl.pallas_call(
        finish,
        name="far_add",
        grid=(count // step,),
        out_shape=jax.ShapeDtypeStruct((count, leaf, width), BF16),
        in_specs=[block_of(leaf, width), block_of(rank, leaf), block_of(rank, width)],
        out_specs=block_of(leaf, width),
        compiler_params=pltpu.CompilerParams(vmem_limit_bytes=63 * 1024 * 1024),
    )(part, jnp.swapaxes(target_basis, 1, 2), far)
    return out.reshape(count * leaf, width)


def solution(mesh):
    in_specs = (
        P("rows", "rhs"),
        P("rows", None, None, None),
        P("rows", None),
        P("rows", None, None),
        P("rows", None, None),
        P("rows", None, None),
        P("rhs", None, None),
        P("rows", None, None, None),
        P("rhs", None, None, None),
        P("rows", None),
        P(),
    )
    out_specs = P("rows", "rhs")
    return jax.shard_map(body, mesh=mesh, in_specs=in_specs, out_specs=out_specs, check_vma=False)
```
